32 devices in a mesh: wide: 8 (over z, y), narrow: 4 (over x, core).
Axes of the slice: x: 2, y: 2, z: 4, core: 2. Of those that a mesh axis runs over, the one named last changes fastest.
Arguments:
- rhs: float32 [3, 32, 32, 128], P(None, 'wide', 'narrow'), may hold values from -12 to 12
- start: float32 [3, 32, 32, 128], P(None, 'wide', 'narrow'), may hold values from -2 to 2
- trans: float32 [3, 32, 32, 128], P(None, 'wide', 'narrow'), may hold values from 0.2 to 2
- accum: float32 [32, 32, 128], P('wide', 'narrow'), may hold values from 2 to 8
- coupling: float32 [3, 3, 32, 32, 128], P(None, None, 'wide', 'narrow'), may hold values from -0.3 to 0.3
- well_cells: int32 [8, 4, 64], P('wide', 'narrow'), may hold values from 0 to 4095
- well_index: float32 [8, 4, 64], P('wide', 'narrow'), may hold values from 1 to 20
- agg_map: int32 [32, 32, 128], P('wide', 'narrow'), may hold values from 0 to 31
- tile_factors: bfloat16 [48, 48, 128, 128], P('wide', 'narrow')
- coarse_inverse: float32 [1024, 1024], P(('wide', 'narrow')), as said below
Outputs:
- iterate: float32 [3, 32, 32, 128], P(None, 'wide', 'narrow')
- residual: float32 [3, 32, 32, 128], P(None, 'wide', 'narrow')
The draws below stay inside these ranges and needn't reach their ends.
Inputs may be any that keep to these rules, and one draw needn't show every extreme that they name: well_cells names, for each device's 64 connections, one of that device's own 4 * 8 * 128 cells, counted by pair, then column, then position in the tile; connections may share a cell. agg_map names one of the 32 aggregates of the device that owns the cell. coarse_inverse is symmetric.
All inputs are finite; a program needn't handle non-finite values.
Results may differ from the reference program's by a relative error of at most 0.00095.
Values sent between devices are 32-bit elements; how exact they have to be, the bound alone decides.
A program may use at most 64 MiB of HBM per device.

```python
import math
import jax
import jax.numpy as jnp
from jax import lax

PHASES = 3
PX = 4
CY = 8
AGG_LOC = 32
CONN = 64
SWEEPS = 3
INNER = 3
TILE = 128
NX2 = 32
NY = 32
TX_ALL = 48
TY_ALL = 48
NAGG = 1024
N_WIDE = 8
N_NARROW = 4


def draw_tile_factors(key, part):
    full_shape = (TX_ALL, TY_ALL, TILE, TILE)
    deviation = 0.02 * jax.random.normal(key, full_shape, jnp.float32)
    return (jnp.eye(TILE, dtype=jnp.float32) + deviation).astype(jnp.bfloat16)


def draw_coarse_inverse(key, part):
    subkeys = jax.random.split(jax.random.fold_in(key, 7), 4)
    owners = NAGG // AGG_LOC
    shuffle = jax.random.permutation(subkeys[0], owners)
    position = jnp.argsort(shuffle)
    partner = shuffle[position ^ 1]
    device_of = jnp.arange(NAGG) // AGG_LOC
    paired = partner[device_of][:, None] == device_of[None, :]
    background = jax.random.normal(subkeys[1], (NAGG, NAGG), jnp.float32)
    partner_part = jax.random.normal(subkeys[2], (NAGG, NAGG), jnp.float32)
    diag_scale = jax.random.uniform(subkeys[3], (NAGG,), jnp.float32, 0.0005, 0.0015)
    back_scale = 5e-06
    sym_back = (background + background.T) * (back_scale / math.sqrt(2.0))
    sym_partner = (partner_part + partner_part.T) * (0.0004 / math.sqrt(2.0))
    return jnp.diag(diag_scale) + sym_back + jnp.where(paired, sym_partner, 0.0)


def set_ends(values, rng, smallest, high):
    longest = values.shape.index(max(values.shape))
    spots = []
    for shift in (0, 1):
        where = [jax.random.randint(jax.random.fold_in(rng, axis), (), 0, length) for axis, length in enumerate(values.shape)]
        where[longest] = (where[longest] + shift) % values.shape[longest]
        spots.append(tuple(where))
    return values.at[spots[0]].set(smallest).at[spots[1]].set(high)


def level_of(rng, shape, shards, least, largest):
    factor_of, own = 1.0, jax.random.fold_in(rng, 6)
    for dim, parts in shards:
        draws = jnp.exp(jax.random.uniform(jax.random.fold_in(own, dim), (parts,), jnp.float32, least / len(shards), largest / len(shards)))
        factor_of = factor_of * jnp.repeat(draws, shape[dim] // parts).reshape([-1 if axis == dim else 1 for axis in range(len(shape))])
    return factor_of


def normal_values(own_key, extent, width, limit, pieces=(), kind=jnp.bfloat16):
    entries = width * jax.random.normal(own_key, extent, jnp.float32)
    if pieces:
        entries = entries * level_of(own_key, extent, pieces, -0.22, 0.18)
    return jnp.clip(entries, -limit, limit).astype(kind)


def setup_inputs(seed: int = 0) -> dict:
    key_of = jax.random.split(jax.random.key(seed), 11)
    rhs = normal_values(key_of[0], (PHASES, NX2, NY, TILE), 2.0, 12.0, ((1, 8), (2, 4)), jnp.float32)
    start = normal_values(key_of[1], (PHASES, NX2, NY, TILE), 0.3, 2.0, ((1, 8), (2, 4)), jnp.float32)
    trans = jnp.clip(jnp.exp(math.log(2.0) - 2.3025851 * jax.random.uniform(key_of[2], (3, NX2, NY, TILE), jnp.float32) ** level_of(key_of[2], (3, NX2, NY, TILE), ((1, 8), (2, 4)), -0.2, 0.2)), 0.2, 2.0)
    accum = jnp.clip(jnp.exp(math.log(8.0) - 1.3862944 * jax.random.uniform(key_of[3], (NX2, NY, TILE), jnp.float32) ** level_of(key_of[3], (NX2, NY, TILE), ((0, 8), (1, 4)), -0.2, 0.2)), 2.0, 8.0)
    coupling = jnp.clip(jax.random.uniform(key_of[4], (PHASES, PHASES, NX2, NY, TILE), jnp.float32, -0.3, 0.3) * level_of(key_of[4], (PHASES, PHASES, NX2, NY, TILE), ((2, 8), (3, 4)), -0.4, 0.0), -0.3, 0.3)
    well_cells = set_ends(jax.random.randint(key_of[5], (N_WIDE, N_NARROW, CONN), 0, PX * CY * TILE), jax.random.fold_in(key_of[5], 1), 0, (PX * CY * TILE) - 1).astype(jnp.int32)
    well_index = jnp.clip(jnp.exp(math.log(20.0) - 2.9957323 * jax.random.uniform(key_of[6], (N_WIDE, N_NARROW, CONN), jnp.float32) ** level_of(key_of[6], (N_WIDE, N_NARROW, CONN), ((0, 8), (1, 4)), -0.2, 0.2)), 1.0, 20.0)
    agg_map = set_ends(jax.random.randint(key_of[7], (NX2, NY, TILE), 0, AGG_LOC), jax.random.fold_in(key_of[7], 1), 0, AGG_LOC - 1).astype(jnp.int32)
    tile_factors = draw_tile_factors(jax.random.fold_in(key_of[10], 71), 0)
    coarse_inverse = draw_coarse_inverse(jax.random.fold_in(key_of[10], 71), 0)
    return {"rhs": rhs, "start": start, "trans": trans, "accum": accum, "coupling": coupling, "well_cells": well_cells, "well_index": well_index, "agg_map": agg_map, "tile_factors": tile_factors, "coarse_inverse": coarse_inverse}


best_precision = lax.Precision.HIGHEST


def neighbour(values, along, offset, periodic):
    along = along % values.ndim
    if periodic:
        return jnp.roll(values, -offset, axis=along)
    length = values.shape[along]
    padding = [(0, 0)] * values.ndim
    if offset > 0:
        padding[along] = (0, offset)
        return lax.slice_in_dim(jnp.pad(values, padding), offset, offset + length, axis=along)
    padding[along] = (-offset, 0)
    return lax.slice_in_dim(jnp.pad(values, padding), 0, length, axis=along)


def east_of(values, periodic):
    middle = values.shape[-1] // 2
    from_next = neighbour(values, -3, 1, periodic)[..., :middle]
    return jnp.concatenate([values[..., middle:], from_next], axis=-1)


def west_of(values, periodic):
    middle = values.shape[-1] // 2
    from_prev = neighbour(values, -3, -1, periodic)[..., middle:]
    return jnp.concatenate([from_prev, values[..., :middle]], axis=-1)


def prepare(trans, accum_w, periodic):
    middle = trans.shape[-1] // 2
    layer_no = lax.broadcasted_iota(jnp.int32, accum_w.shape, accum_w.ndim - 1) % middle
    trans_x = trans[0]
    trans_y = trans[1]
    trans_z = jnp.where(layer_no < middle - 1, trans[2], 0.0)
    face_sum = trans_x + west_of(trans_x, periodic) + trans_y + neighbour(trans_y, -2, -1, periodic)
    face_sum = face_sum + trans_z + neighbour(trans_z, -1, -1, False)
    return trans_x, trans_y, trans_z, accum_w + face_sum


def operate(values, trans_x, trans_y, trans_z, centre, coupling, periodic):
    mixing = jnp.sum(coupling * values[None], axis=1)
    inflow = trans_x * east_of(values, periodic) + west_of(trans_x, periodic) * west_of(values, periodic)
    inflow = inflow + trans_y * neighbour(values, -2, 1, periodic)
    inflow = inflow + neighbour(trans_y, -2, -1, periodic) * neighbour(values, -2, -1, periodic)
    inflow = inflow + trans_z * neighbour(values, -1, 1, False)
    inflow = inflow + neighbour(trans_z, -1, -1, False) * neighbour(values, -1, -1, False)
    return centre * values + mixing - inflow


def tile_apply(values, inverse_diag, factors):
    scaled = (inverse_diag * values).astype(jnp.bfloat16)
    return jnp.einsum("cpyj,pykj->cpyk", scaled.astype(jnp.float32), factors.astype(jnp.float32), precision=best_precision)


def local_solve(misfit, coeffs, inverse_diag, factors):
    trans_x, trans_y, trans_z, centre, coupling = coeffs
    update = tile_apply(misfit, inverse_diag, factors)
    for _ in range(INNER - 1):
        applied = operate(update, trans_x, trans_y, trans_z, centre, coupling, False)
        update = update + tile_apply(misfit - applied, inverse_diag, factors)
    return update


def wrap_pad(values):
    widths = ((1, 1), (2, 2), (0, 0))
    return jnp.pad(values, ((0, 0),) * (values.ndim - 3) + widths, mode="wrap")


def subdomains(misfit_pad, padded, tile_factors):
    def one_device(device_no):
        wide_pos = (device_no // N_NARROW).astype(jnp.int32)
        narrow_pos = (device_no % N_NARROW).astype(jnp.int32)
        zero = jnp.zeros((), jnp.int32)

        def window(values):
            cut_x = lax.dynamic_slice_in_dim(values, (wide_pos * PX).astype(jnp.int32), PX + 2, values.ndim - 3)
            return lax.dynamic_slice_in_dim(cut_x, (narrow_pos * CY).astype(jnp.int32), CY + 4, values.ndim - 2)

        coeffs = [window(member) for member in padded[:5]]
        starts = ((wide_pos * (PX + 2)).astype(jnp.int32), (narrow_pos * (CY + 4)).astype(jnp.int32), zero, zero)
        factors = lax.dynamic_slice(tile_factors, starts, (PX + 2, CY + 4, TILE, TILE))
        update = local_solve(window(misfit_pad), coeffs, window(padded[5]), factors)
        return update[:, 1:-1, 2:-2, :]

    blocks = lax.map(one_device, jnp.arange(N_WIDE * N_NARROW, dtype=jnp.int32))
    blocks = blocks.reshape(N_WIDE, N_NARROW, PHASES, PX, CY, TILE)
    return blocks.transpose(2, 0, 3, 1, 4, 5).reshape(PHASES, N_WIDE * PX, N_NARROW * CY, TILE)


def reference(rhs, start, trans, accum, coupling, well_cells, well_index, agg_map, tile_factors, coarse_inverse):
    flat_local = well_cells.astype(jnp.int32)
    pair_pos = jnp.arange(N_WIDE, dtype=jnp.int32)[:, None, None] * PX + flat_local // (CY * TILE)
    row_pos = jnp.arange(N_NARROW, dtype=jnp.int32)[None, :, None] * CY + (flat_local // TILE) % CY
    cell_pos = flat_local % TILE
    accum_w = accum.at[pair_pos, row_pos, cell_pos].add(well_index)
    trans_x, trans_y, trans_z, centre = prepare(trans, accum_w, True)
    coupling_diag = jnp.stack([coupling[member, member] for member in range(PHASES)])
    inverse_diag = 1.0 / (centre[None] + coupling_diag)
    padded = [wrap_pad(member) for member in (trans_x, trans_y, trans_z, centre, coupling, inverse_diag)]
    owner_no = (lax.broadcasted_iota(jnp.int32, accum.shape, 0) // PX) * N_NARROW
    owner_no = owner_no + lax.broadcasted_iota(jnp.int32, accum.shape, 1) // CY
    group_ids = (owner_no * AGG_LOC + agg_map.astype(jnp.int32)).reshape(-1)
    current = start
    for _ in range(SWEEPS):
        misfit = rhs - operate(current, trans_x, trans_y, trans_z, centre, coupling, True)
        correction = subdomains(wrap_pad(misfit), padded, tile_factors)
        coarse_rhs = jax.ops.segment_sum(misfit[0].reshape(-1), group_ids, num_segments=NAGG)
        coarse_sol = jnp.dot(coarse_inverse, coarse_rhs, precision=best_precision)
        correction = correction.at[0].add(coarse_sol[group_ids].reshape(accum.shape))
        current = current + correction
    final_misfit = rhs - operate(current, trans_x, trans_y, trans_z, centre, coupling, True)
    return current, final_misfit
```

```python
import functools

import jax
import jax.numpy as jnp
from jax import lax
from jax.experimental import pallas as pl
from jax.experimental.pallas import tpu as pltpu
from jax.sharding import PartitionSpec as P

SWEEPS = 3
HIGHEST = lax.Precision.HIGHEST
NT = (((1,), (1,)), ((), ()))
F32 = jnp.float32

DIRS = ((-1, 0), (1, 0), (0, -1), (0, 1), (-1, -1), (-1, 1), (1, -1), (1, 1))


def halo_pieces(px, cy, depth_x, depth_y):
    pieces = []
    for dx, dy in DIRS:
        if dx == 0:
            sp, dp, np_ = 2, 2, px
        elif dx > 0:
            sp, dp, np_ = 2 + px - depth_x, 2 - depth_x, depth_x
        else:
            sp, dp, np_ = 2, 2 + px, depth_x
        if dy == 0:
            sr, dr, nr = 0, 0, cy
        elif dy > 0:
            sr, dr, nr = cy - depth_y, 2 * cy - depth_y, depth_y
        else:
            sr, dr, nr = 0, cy, depth_y
        pieces.append(((sp, sr), (dp, dr), (np_, nr)))
    return pieces


def body(
    nw, nn,
    rhs, start, trans, accum, coupling, cells, widx, agg, tiles, cinv,
    out_it, out_res,
    COEF, CUR, W1, W2, H, DER, TF, CI, AG, ACC, GN, GW, XN, XW,
    loc, hs, hr, cs, cr, ns, nr, ws, wr,
):
    phases = rhs.shape[0]
    px, cy, tile = accum.shape
    box = px + 2
    half = tile // 2
    aggs = CI.shape[0]
    me_w, me_n = lax.axis_index("wide"), lax.axis_index("narrow")

    def dev(dw, dn):
        return {"wide": lax.rem(me_w + dw + nw, nw), "narrow": lax.rem(me_n + dn + nn, nn)}

    own = pl.ds(2, px)
    top = pl.ds(0, cy)
    nch = COEF.shape[0]
    first_rhs = nch - phases
    copies = [
        (accum, ACC),
        (trans, COEF.at[pl.ds(0, 3), own, top]),
        (start, CUR.at[0, :, own, top]),
        (coupling, COEF.at[pl.ds(4, phases * phases), own, top]),
        (rhs, COEF.at[pl.ds(first_rhs, phases), own, top]),
        (agg, AG),
        (cinv, CI),
        (tiles, TF),
    ]
    local = [pltpu.make_async_copy(s, d, loc.at[k]) for k, (s, d) in enumerate(copies)]
    for c in local:
        c.start()

    barrier = pltpu.get_barrier_semaphore()
    peers = [(0, d) for d in range(1, nn)] + [(d, 0) for d in range(1, nw)]
    peers += [d for d in DIRS if d[0] and d[1]]
    for d in peers:
        pl.semaphore_signal(barrier, inc=1, device_id=dev(*d), device_id_type=pl.DeviceIdType.MESH)

    conn = cells.shape[-1]
    cell_row = cells[...]
    rows_own = px * cy
    hit_r = lax.broadcasted_iota(jnp.int32, (rows_own, conn), 0) == cell_row // tile
    hit_l = lax.broadcasted_iota(jnp.int32, (tile, conn), 0) == cell_row % tile
    left = jnp.where(hit_r, jnp.broadcast_to(widx[...], (rows_own, conn)), 0.0)
    right = jnp.where(hit_l, 1.0, 0.0)
    wells = lax.dot_general(left, right, NT, precision=HIGHEST, preferred_element_type=F32)
    local[0].wait()
    COEF[3, 2 : 2 + px, 0:cy, :] = ACC[...] + wells.reshape(px, cy, tile)
    for c in local[1:5]:
        c.wait()
    pl.semaphore_wait(barrier, len(peers))

    def remote(src, dst, ss, rs, d):
        return pltpu.make_async_remote_copy(
            src_ref=src, dst_ref=dst, send_sem=ss, recv_sem=rs,
            device_id=dev(*d), device_id_type=pl.DeviceIdType.MESH,
        )

    pieces = halo_pieces(px, cy, 2, 3)

    def halo(e):
        out = []
        for k, d in enumerate(DIRS):
            (sp, sr), (dp, dr), (npair, nrow) = pieces[k]
            out.append(remote(
                CUR.at[e, :, pl.ds(sp, npair), pl.ds(sr, nrow)],
                CUR.at[e, :, pl.ds(dp, npair), pl.ds(dr, nrow)],
                hs.at[e, k], hr.at[e, k], d))
        return out

    coef = []
    for k, d in enumerate(DIRS):
        (sp, sr), (dp, dr), (npair, nrow) = halo_pieces(px, cy, 1, 3)[k]
        coef.append(remote(
            COEF.at[:, pl.ds(sp, npair), pl.ds(sr, nrow)],
            COEF.at[:, pl.ds(dp, npair), pl.ds(dr, nrow)],
            cs.at[k], cr.at[k], d))
    extra = len(DIRS)
    for k, d in enumerate(DIRS):
        if d[0] > 0:
            (sp, sr), (dp, dr), (npair, nrow) = pieces[k]
            coef.append(remote(
                COEF.at[pl.ds(0, 1), pl.ds(sp, 1), pl.ds(sr, nrow)],
                COEF.at[pl.ds(0, 1), pl.ds(dp, 1), pl.ds(dr, nrow)],
                cs.at[extra], cr.at[extra], d))
            extra += 1
    for c in halo(0) + coef:
        c.start()

    lane = lax.broadcasted_iota(jnp.int32, (2 * cy, tile), 1)
    low = lane < half
    roll = pltpu.roll

    zero16 = jnp.zeros((2 * cy, tile), F32)
    for c in range(phases):
        for w in (W1, W2):
            w[c, 0] = zero16
            w[c, box + 1] = zero16
        W2[c, 1] = zero16
        W2[c, box] = zero16
    for c in local[5:]:
        c.wait()
    for c in coef:
        c.wait_recv()

    for b in range(box):
        tx = COEF[0, b + 1]
        txw = jnp.where(low, roll(COEF[0, b], half, 1), roll(tx, half, 1))
        ty = COEF[1, b + 1]
        tys = roll(ty, 1, 0)
        tz = jnp.where(lane % half < half - 1, COEF[2, b + 1], 0.0)
        tzd = roll(tz, 1, 1)
        centre = COEF[3, b + 1] + (tx + txw + ty + tys + tz + tzd)
        DER[0, b] = txw
        DER[1, b] = tys
        DER[2, b] = tz
        DER[3, b] = tzd
        for c in range(phases):
            diag = centre + COEF[4 + c * phases + c, b + 1]
            DER[4 + c, b] = diag
            DER[4 + phases + c, b] = 1.0 / diag

    def operate(read, boxes):
        swapped = {}

        def swap(c, idx):
            if (c, idx) not in swapped:
                swapped[c, idx] = roll(read(c, idx), half, 1)
            return swapped[c, idx]

        for b in boxes:
            values = [read(c, b + 1) for c in range(phases)]
            result = []
            for c in range(phases):
                v = values[c]
                east = jnp.where(low, swap(c, b + 1), swap(c, b + 2))
                west = jnp.where(low, swap(c, b), swap(c, b + 1))
                total = DER[4 + c, b] * v
                for o in range(phases):
                    if o != c:
                        total = total + COEF[4 + c * phases + o, b + 1] * values[o]
                inflow = COEF[0, b + 1] * east + DER[0, b] * west
                inflow = inflow + COEF[1, b + 1] * roll(v, 2 * cy - 1, 0)
                inflow = inflow + DER[1, b] * roll(v, 1, 0)
                inflow = inflow + DER[2, b] * roll(v, tile - 1, 1)
                inflow = inflow + DER[3, b] * roll(v, 1, 1)
                result.append(total - inflow)
            yield b, result

    row = lax.broadcasted_iota(jnp.int32, (phases * cy, tile), 0) % cy

    def product(b, q, chosen):
        stack = jnp.concatenate(q, axis=0)
        lhs = jnp.concatenate(
            [jnp.where(row == r, stack, 0.0) for r, _ in chosen], axis=1).astype(jnp.bfloat16)
        factors = jnp.concatenate([TF[b, t] for _, t in chosen], axis=1)
        out = lax.dot_general(lhs, factors, NT, preferred_element_type=F32)
        return [out[c * cy : (c + 1) * cy] for c in range(phases)]

    ring_a = tuple((y, y + 2) for y in range(cy))
    ring_b = ((0, cy + 2), (1, cy + 3), (cy - 2, 0), (cy - 1, 1))
    near_b = ((0, cy + 2), (cy - 1, 1))
    inner = range(1, box - 1)

    def scaled(b, h):
        return [DER[4 + phases + c, b] * h[c] for c in range(phases)]

    agg_iota = lax.broadcasted_iota(jnp.int32, (aggs, tile), 0)
    lane8 = lax.broadcasted_iota(jnp.int32, (cy, tile), 1)
    ones = jnp.ones((cy, tile), F32)

    def sweep(s, carry):
        for c in halo(s):
            c.wait_recv()
        acc = jnp.zeros((aggs, tile), F32)
        for b, applied in operate(lambda c, idx: CUR[s, c, idx], range(box)):
            h = [COEF[first_rhs + c, b + 1] - applied[c] for c in range(phases)]
            for c in range(phases):
                H[c, b] = h[c]
            if b in inner:
                for y in range(cy):
                    ids = AG[pl.ds((b - 1) * cy + y, 1), :]
                    acc = acc + jnp.where(agg_iota == ids, h[0][y : y + 1], 0.0)
        wide_acc = jnp.concatenate([acc] * (tile // aggs), axis=0)
        XN[s] = lax.dot_general(ones, wide_acc, NT, precision=HIGHEST, preferred_element_type=F32)
        near = [remote(XN.at[s], GN.at[s, d - 1], ns.at[s, d - 1], nr.at[s, d - 1], (0, d))
                for d in range(1, nn)]
        for c in near:
            c.start()

        for b in range(box):
            q = scaled(b, [H[c, b] for c in range(phases)])
            upper = product(b, [v[:cy] for v in q], ring_a)
            lower = product(b, [v[cy:] for v in q], ring_b if b in inner else near_b)
            for c in range(phases):
                W1[c, b + 1, 0:cy] = upper[c]
                W1[c, b + 1, cy : 2 * cy] = lower[c]

        for c in near:
            c.wait_recv()
        owner = lane8 // aggs
        line = XN[s]
        for d in range(1, nn):
            line = jnp.where(owner == lax.rem(me_n - d + nn, nn), GN[s, d - 1], line)
        XW[s] = line
        far = [remote(XW.at[s], GW.at[s, d - 1], ws.at[s, d - 1], wr.at[s, d - 1], (d, 0))
               for d in range(1, nw)]
        for c in far:
            c.start()

        for b, applied in operate(lambda c, idx: W1[c, idx], range(box)):
            q = scaled(b, [H[c, b] - applied[c] for c in range(phases)])
            upper = product(b, [v[:cy] for v in q], ring_a)
            for c in range(phases):
                W2[c, b + 1, 0:cy] = W1[c, b + 1, 0:cy] + upper[c]
            if b in inner:
                lower = product(b, [v[cy:] for v in q], near_b)
                for c in range(phases):
                    W2[c, b + 1, cy : 2 * cy] = W1[c, b + 1, cy : 2 * cy] + lower[c]

        for b, applied in operate(lambda c, idx: W2[c, idx], inner):
            q = scaled(b, [H[c, b] - applied[c] for c in range(phases)])
            upper = product(b, [v[:cy] for v in q], ring_a)
            for c in range(phases):
                W1[c, b + 1, 0:cy] = W2[c, b + 1, 0:cy] + upper[c]

        for c in far:
            c.wait_recv()

        def weight(g, d):
            return CI[:, pl.ds(pl.multiple_of(g * tile, tile), tile)] * jnp.concatenate(
                [d] * (aggs // cy), axis=0)

        part = weight(me_w, XW[s])
        for d in range(1, nw):
            part = part + weight(lax.rem(me_w - d + nw, nw), GW[s, d - 1])
        sol = lax.dot_general(ones, part, NT, precision=HIGHEST, preferred_element_type=F32)
        ids = AG[...]
        lifted = jnp.zeros((rows_own, tile), F32)
        for g in range(aggs):
            value = jnp.broadcast_to(sol[0:1, g : g + 1], (rows_own, tile))
            lifted = jnp.where(ids == g, value, lifted)
        for c in range(phases):
            for p in range(px):
                new = CUR[s, c, p + 2, 0:cy] + W1[c, p + 2, 0:cy]
                if c == 0:
                    new = new + lifted[p * cy : (p + 1) * cy]
                CUR[s + 1, c, p + 2, 0:cy] = new
        for c in halo(s + 1):
            c.start()
        for c in near + far:
            c.wait_send()
        for c in halo(s):
            c.wait_send()
        return carry

    lax.fori_loop(0, SWEEPS, sweep, 0)
    for c in range(phases):
        out_it[c] = CUR[SWEEPS, c, 2 : 2 + px, 0:cy]
    for c in halo(SWEEPS):
        c.wait_recv()
    for b, applied in operate(lambda c, idx: CUR[SWEEPS, c, idx], inner):
        for c in range(phases):
            out_res[c, b - 1] = COEF[first_rhs + c, b + 1, 0:cy] - applied[c][:cy]
    for c in halo(SWEEPS) + coef:
        c.wait_send()


def solution(mesh):
    nw, nn = mesh.shape["wide"], mesh.shape["narrow"]

    def per_device(rhs, start, trans, accum, coupling, well_cells, well_index, agg_map, tile_factors, coarse_inverse):
        phases, px, cy, tile = rhs.shape
        box = px + 2
        aggs = coarse_inverse.shape[0]
        nch = 4 + phases * phases + phases
        vmem = pl.BlockSpec(memory_space=pltpu.VMEM)
        hbm = pl.BlockSpec(memory_space=pl.ANY)
        shape = jax.ShapeDtypeStruct(rhs.shape, F32)
        ring = (2 * cy, tile)
        dma = pltpu.SemaphoreType.DMA
        call = pl.pallas_call(
            functools.partial(body, nw, nn),
            out_shape=(shape, shape),
            in_specs=[hbm, hbm, hbm, hbm, hbm, vmem, vmem, hbm, hbm, hbm],
            out_specs=(vmem, vmem),
            scratch_shapes=[
                pltpu.VMEM((nch, px + 4) + ring, F32),
                pltpu.VMEM((SWEEPS + 1, phases, px + 4) + ring, F32),
                pltpu.VMEM((phases, px + 4) + ring, F32),
                pltpu.VMEM((phases, px + 4) + ring, F32),
                pltpu.VMEM((phases, box) + ring, F32),
                pltpu.VMEM((4 + 2 * phases, box) + ring, F32),
                pltpu.VMEM(tile_factors.shape, tile_factors.dtype),
                pltpu.VMEM(coarse_inverse.shape, F32),
                pltpu.VMEM((px * cy, tile), jnp.int32),
                pltpu.VMEM(accum.shape, F32),
                pltpu.VMEM((SWEEPS, nn - 1, cy, tile), F32),
                pltpu.VMEM((SWEEPS, nw - 1, cy, tile), F32),
                pltpu.VMEM((SWEEPS, cy, tile), F32),
                pltpu.VMEM((SWEEPS, cy, tile), F32),
                dma((8,)),
                dma((SWEEPS + 1, len(DIRS))),
                dma((SWEEPS + 1, len(DIRS))),
                dma((len(DIRS) + 3,)),
                dma((len(DIRS) + 3,)),
                dma((SWEEPS, nn - 1)),
                dma((SWEEPS, nn - 1)),
                dma((SWEEPS, nw - 1)),
                dma((SWEEPS, nw - 1)),
            ],
            compiler_params=pltpu.CompilerParams(collective_id=0, has_side_effects=True),
            name="schwarz",
        )
        return call(
            rhs, start, trans, accum,
            coupling.reshape((phases * phases,) + accum.shape),
            well_cells.reshape(1, -1), well_index.reshape(1, -1),
            agg_map.reshape(px * cy, tile), tile_factors, coarse_inverse)

    return jax.shard_map(
        per_device,
        mesh=mesh,
        in_specs=(
            P(None, "wide", "narrow", None),
            P(None, "wide", "narrow", None),
            P(None, "wide", "narrow", None),
            P("wide", "narrow", None),
            P(None, None, "wide", "narrow", None),
            P("wide", "narrow", None),
            P("wide", "narrow", None),
            P("wide", "narrow", None),
            P("wide", "narrow", None, None),
            P(("wide", "narrow"), None),
        ),
        out_specs=(P(None, "wide", "narrow", None), P(None, "wide", "narrow", None)),
        check_vma=False,
    )
```

```python
import functools

import jax
import jax.numpy as jnp
from jax import lax
from jax.experimental import pallas as pl
from jax.experimental.pallas import tpu as pltpu
from jax.sharding import PartitionSpec as P

SWEEPS = 3
HIGHEST = lax.Precision.HIGHEST
NT = (((1,), (1,)), ((), ()))
F32 = jnp.float32

DIRS = ((-1, 0), (1, 0), (0, -1), (0, 1), (-1, -1), (-1, 1), (1, -1), (1, 1))


def halo_piece(d, px, cy, depth_x, depth_y):
    dx, dy = d
    if dx == 0:
        sp, dp, npair = 2, 2, px
    elif dx > 0:
        sp, dp, npair = 2 + px - depth_x, 2 - depth_x, depth_x
    else:
        sp, dp, npair = 2, 2 + px, depth_x
    if dy == 0:
        sr, dr, nrow = 0, 0, cy
    elif dy > 0:
        sr, dr, nrow = cy - depth_y, 2 * cy - depth_y, depth_y
    else:
        sr, dr, nrow = 0, cy, depth_y
    return (pl.ds(sp, npair), pl.ds(sr, nrow)), (pl.ds(dp, npair), pl.ds(dr, nrow))


def body(
    nw, nn,
    rhs, start, trans, accum, coupling, cells, widx, agg, tiles, cinv,
    out_it, out_res,
    COEF, CUR, FIX, W1, W2, H, DER, TF, CI, AG, AGX, ACC, GB, YB,
    loc, hs, hr, cs, cr, gs, gr, is_, ir,
):
    phases = rhs.shape[0]
    px, cy, tile = accum.shape
    box = px + 2
    half = tile // 2
    aggs = CI.shape[0]
    me_w, me_n = lax.axis_index("wide"), lax.axis_index("narrow")

    def dev(dw, dn):
        return {"wide": lax.rem(me_w + dw + nw, nw), "narrow": lax.rem(me_n + dn + nn, nn)}

    own = pl.ds(2, px)
    top = pl.ds(0, cy)
    nch = COEF.shape[0]
    first_rhs = nch - phases
    copies = [
        (accum, ACC),
        (trans, COEF.at[pl.ds(0, 3), own, top]),
        (start, CUR.at[0, :, own, top]),
        (coupling, COEF.at[pl.ds(4, phases * phases), own, top]),
        (rhs, COEF.at[pl.ds(first_rhs, phases), own, top]),
        (agg, AG),
        (cinv, CI),
        (tiles, TF),
    ]
    local = [pltpu.make_async_copy(s, d, loc.at[k]) for k, (s, d) in enumerate(copies)]
    for c in local:
        c.start()

    barrier = pltpu.get_barrier_semaphore()
    peers = [(dw, dn) for dw in range(nw) for dn in range(nn) if dw or dn]
    for p in range(px + 4):
        AGX[p] = jnp.zeros((2 * cy, tile), jnp.int32)
    for d in peers:
        pl.semaphore_signal(barrier, inc=1, device_id=dev(*d), device_id_type=pl.DeviceIdType.MESH)

    conn = cells.shape[-1]
    cell_row = cells[...]
    rows_own = px * cy
    hit_r = lax.broadcasted_iota(jnp.int32, (rows_own, conn), 0) == cell_row // tile
    hit_l = lax.broadcasted_iota(jnp.int32, (tile, conn), 0) == cell_row % tile
    left = jnp.where(hit_r, jnp.broadcast_to(widx[...], (rows_own, conn)), 0.0)
    right = jnp.where(hit_l, 1.0, 0.0)
    wells = lax.dot_general(left, right, NT, precision=HIGHEST, preferred_element_type=F32)
    local[0].wait()
    COEF[3, 2 : 2 + px, 0:cy, :] = ACC[...] + wells.reshape(px, cy, tile)
    for c in local[1:5]:
        c.wait()
    pl.semaphore_wait(barrier, len(peers))

    def remote(src, dst, ss, rs, d):
        return pltpu.make_async_remote_copy(
            src_ref=src, dst_ref=dst, send_sem=ss, recv_sem=rs,
            device_id=dev(*d), device_id_type=pl.DeviceIdType.MESH,
        )

    def halo(e):
        out = []
        for k, d in enumerate(DIRS):
            src, dst = halo_piece(d, px, cy, 2, 2 if d[0] else 3)
            out.append(remote(CUR.at[(e, slice(None)) + src], CUR.at[(e, slice(None)) + dst],
                              hs.at[e, k], hr.at[e, k], d))
        return out

    coef = []

    def send_coef(channels, src, dst, d):
        k = len(coef)
        coef.append(remote(COEF.at[(channels,) + src], COEF.at[(channels,) + dst], cs.at[k], cr.at[k], d))

    for d in DIRS:
        depth_y = 1 if d[0] < 0 else 2
        src, dst = halo_piece(d, px, cy, 1, depth_y)
        send_coef(pl.ds(0, nch), src, dst, d)
        if d[0] > 0:
            (_, sr), (_, dr) = src, dst
            send_coef(pl.ds(0, 1), (pl.ds(px, 1), sr), (pl.ds(0, 1), dr), d)
        if d[1] > 0:
            (sp, _), (dp, _) = src, dst
            send_coef(pl.ds(1, 1), (sp, pl.ds(cy - depth_y - 1, 1)), (dp, pl.ds(2 * cy - depth_y - 1, 1)), d)

    aggregates = []
    for k, d in enumerate(DIRS):
        src, dst = halo_piece(d, px, cy, 2, 2 if d[0] else 3)
        aggregates.append(remote(AGX.at[src], AGX.at[dst], is_.at[k], ir.at[k], d))
    for c in halo(0) + coef:
        c.start()
    local[5].wait()
    AGX[2 : 2 + px, 0:cy] = (AG[...] + me_n * aggs).reshape(px, cy, tile)
    for c in aggregates:
        c.start()

    lane = lax.broadcasted_iota(jnp.int32, (2 * cy, tile), 1)
    low = lane < half
    roll = pltpu.roll

    zero16 = jnp.zeros((2 * cy, tile), F32)
    for c in range(phases):
        for w in (W1, W2):
            w[c, 0] = zero16
            w[c, box + 1] = zero16
        W2[c, 1] = zero16
        W2[c, box] = zero16
    for c in local[6:]:
        c.wait()
    for c in coef:
        c.wait_recv()

    for b in range(box):
        tx = COEF[0, b + 1]
        txw = jnp.where(low, roll(COEF[0, b], half, 1), roll(tx, half, 1))
        ty = COEF[1, b + 1]
        tys = roll(ty, 1, 0)
        tz = jnp.where(lane % half < half - 1, COEF[2, b + 1], 0.0)
        tzd = roll(tz, 1, 1)
        centre = COEF[3, b + 1] + (tx + txw + ty + tys + tz + tzd)
        DER[0, b] = txw
        DER[1, b] = tys
        DER[2, b] = tz
        DER[3, b] = tzd
        for c in range(phases):
            diag = centre + COEF[4 + c * phases + c, b + 1]
            DER[4 + c, b] = diag
            DER[4 + phases + c, b] = 1.0 / diag

    def operate(read, boxes):
        swapped = {}

        def swap(c, idx):
            if (c, idx) not in swapped:
                swapped[c, idx] = roll(read(c, idx), half, 1)
            return swapped[c, idx]

        for b in boxes:
            values = [read(c, b + 1) for c in range(phases)]
            result = []
            for c in range(phases):
                v = values[c]
                east = jnp.where(low, swap(c, b + 1), swap(c, b + 2))
                west = jnp.where(low, swap(c, b), swap(c, b + 1))
                total = DER[4 + c, b] * v
                for o in range(phases):
                    if o != c:
                        total = total + COEF[4 + c * phases + o, b + 1] * values[o]
                inflow = COEF[0, b + 1] * east + DER[0, b] * west
                inflow = inflow + COEF[1, b + 1] * roll(v, 2 * cy - 1, 0)
                inflow = inflow + DER[1, b] * roll(v, 1, 0)
                inflow = inflow + DER[2, b] * roll(v, tile - 1, 1)
                inflow = inflow + DER[3, b] * roll(v, 1, 1)
                result.append(total - inflow)
            yield b, result

    row = lax.broadcasted_iota(jnp.int32, (phases * cy, tile), 0) % cy

    def product(b, q, chosen):
        stack = jnp.concatenate(q, axis=0)
        lhs = jnp.concatenate(
            [jnp.where(row == r, stack, 0.0) for r, _ in chosen], axis=1).astype(jnp.bfloat16)
        factors = jnp.concatenate([TF[b, t] for _, t in chosen], axis=1)
        out = lax.dot_general(lhs, factors, NT, preferred_element_type=F32)
        return [out[c * cy : (c + 1) * cy] for c in range(phases)]

    ring_a = tuple((y, y + 2) for y in range(cy))
    ring_b = ((0, cy + 2), (1, cy + 3), (cy - 2, 0), (cy - 1, 1))
    near_b = ((0, cy + 2), (cy - 1, 1))
    inner = range(1, box - 1)

    def scaled(b, h):
        return [DER[4 + phases + c, b] * h[c] for c in range(phases)]

    agg_iota = lax.broadcasted_iota(jnp.int32, (aggs, tile), 0)

    def current(e):
        return lambda c, idx: FIX[idx] if c == 0 else CUR[e, c, idx]

    def sweep(s, carry):
        read = current(s)
        acc = jnp.zeros((aggs, tile), F32)
        order = list(inner) + [0, box - 1]
        for b, applied in operate(read, order):
            h = [COEF[first_rhs + c, b + 1] - applied[c] for c in range(phases)]
            for c in range(phases):
                H[c, b] = h[c]
            if b in inner:
                for y in range(cy):
                    ids = AG[pl.ds((b - 1) * cy + y, 1), :]
                    acc = acc + jnp.where(agg_iota == ids, h[0][y : y + 1], 0.0)
        sums = jnp.broadcast_to(jnp.sum(acc, axis=1, keepdims=True), (aggs, tile))
        for g in range(nw):
            y = jnp.sum(CI[:, g * tile : (g + 1) * tile] * sums, axis=0, keepdims=True)
            for k in range(3):
                YB[s, (g + 1 - k) % nw, k : k + 1] = y
        share = [remote(YB.at[s, lax.rem(me_w + d[0], nw)], GB.at[s, k], gs.at[k], gr.at[s, k], d)
                 for k, d in enumerate(peers)]
        for c in share:
            c.start()

        for b in range(box):
            q = scaled(b, [H[c, b] for c in range(phases)])
            upper = product(b, [v[:cy] for v in q], ring_a)
            lower = product(b, [v[cy:] for v in q], ring_b if b in inner else near_b)
            for c in range(phases):
                W1[c, b + 1, 0:cy] = upper[c]
                W1[c, b + 1, cy : 2 * cy] = lower[c]

        for b, applied in operate(lambda c, idx: W1[c, idx], range(box)):
            q = scaled(b, [H[c, b] - applied[c] for c in range(phases)])
            upper = product(b, [v[:cy] for v in q], ring_a)
            for c in range(phases):
                W2[c, b + 1, 0:cy] = W1[c, b + 1, 0:cy] + upper[c]
            if b in inner:
                lower = product(b, [v[cy:] for v in q], near_b)
                for c in range(phases):
                    W2[c, b + 1, cy : 2 * cy] = W1[c, b + 1, cy : 2 * cy] + lower[c]

        for b, applied in operate(lambda c, idx: W2[c, idx], inner):
            q = scaled(b, [H[c, b] - applied[c] for c in range(phases)])
            upper = product(b, [v[:cy] for v in q], ring_a)
            for c in range(phases):
                W1[c, b + 1, 0:cy] = W2[c, b + 1, 0:cy] + upper[c]

        for c in range(phases):
            for p in range(px):
                CUR[s + 1, c, p + 2, 0:cy] = read(c, p + 2)[:cy] + W1[c, p + 2, 0:cy]
        for c in halo(s + 1):
            c.start()
        for c in share:
            c.wait_recv()
        total = YB[s, me_w]
        for k in range(len(peers)):
            total = total + GB[s, k]
        tables = [jnp.broadcast_to(total[k : k + 1], (2 * cy, tile)) for k in range(3)]
        for c in halo(s + 1):
            c.wait_recv()
        for p in range(px + 4):
            table = tables[0 if p < 2 else 1 if p < 2 + px else 2]
            lifted = jnp.take_along_axis(table, AGX[p], axis=1, mode="promise_in_bounds")
            FIX[p] = CUR[s + 1, 0, p] + lifted
        for c in share + halo(s):
            c.wait_send()
        return carry

    for c in halo(0):
        c.wait_recv()
    for p in range(px + 4):
        FIX[p] = CUR[0, 0, p]
    for c in aggregates:
        c.wait_recv()
    lax.fori_loop(0, SWEEPS, sweep, 0)
    last = current(SWEEPS)
    for c in range(phases):
        for p in range(px):
            out_it[c, p] = last(c, p + 2)[:cy]
    for b, applied in operate(last, inner):
        for c in range(phases):
            out_res[c, b - 1] = COEF[first_rhs + c, b + 1, 0:cy] - applied[c][:cy]
    for c in halo(SWEEPS) + coef + aggregates:
        c.wait_send()


def solution(mesh):
    nw, nn = mesh.shape["wide"], mesh.shape["narrow"]

    def per_device(rhs, start, trans, accum, coupling, well_cells, well_index, agg_map, tile_factors, coarse_inverse):
        phases, px, cy, tile = rhs.shape
        box = px + 2
        aggs = coarse_inverse.shape[0]
        nch = 4 + phases * phases + phases
        vmem = pl.BlockSpec(memory_space=pltpu.VMEM)
        hbm = pl.BlockSpec(memory_space=pl.ANY)
        shape = jax.ShapeDtypeStruct(rhs.shape, F32)
        ring = (2 * cy, tile)
        dma = pltpu.SemaphoreType.DMA
        call = pl.pallas_call(
            functools.partial(body, nw, nn),
            out_shape=(shape, shape),
            in_specs=[hbm, hbm, hbm, hbm, hbm, vmem, vmem, hbm, hbm, hbm],
            out_specs=(vmem, vmem),
            scratch_shapes=[
                pltpu.VMEM((nch, px + 4) + ring, F32),
                pltpu.VMEM((SWEEPS + 1, phases, px + 4) + ring, F32),
                pltpu.VMEM((px + 4,) + ring, F32),
                pltpu.VMEM((phases, px + 4) + ring, F32),
                pltpu.VMEM((phases, px + 4) + ring, F32),
                pltpu.VMEM((phases, box) + ring, F32),
                pltpu.VMEM((4 + 2 * phases, box) + ring, F32),
                pltpu.VMEM(tile_factors.shape, tile_factors.dtype),
                pltpu.VMEM(coarse_inverse.shape, F32),
                pltpu.VMEM((px * cy, tile), jnp.int32),
                pltpu.VMEM((px + 4,) + ring, jnp.int32),
                pltpu.VMEM(accum.shape, F32),
                pltpu.VMEM((SWEEPS, nw * nn - 1, 3, tile), F32),
                pltpu.VMEM((SWEEPS, nw, 3, tile), F32),
                dma((8,)),
                dma((SWEEPS + 1, len(DIRS))),
                dma((SWEEPS + 1, len(DIRS))),
                dma((14,)),
                dma((14,)),
                dma((nw * nn - 1,)),
                dma((SWEEPS, nw * nn - 1)),
                dma((len(DIRS),)),
                dma((len(DIRS),)),
            ],
            compiler_params=pltpu.CompilerParams(collective_id=0, has_side_effects=True),
            name="schwarz",
        )
        return call(
            rhs, start, trans, accum,
            coupling.reshape((phases * phases,) + accum.shape),
            well_cells.reshape(1, -1), well_index.reshape(1, -1),
            agg_map.reshape(px * cy, tile), tile_factors, coarse_inverse)

    return jax.shard_map(
        per_device,
        mesh=mesh,
        in_specs=(
            P(None, "wide", "narrow", None),
            P(None, "wide", "narrow", None),
            P(None, "wide", "narrow", None),
            P("wide", "narrow", None),
            P(None, None, "wide", "narrow", None),
            P("wide", "narrow", None),
            P("wide", "narrow", None),
            P("wide", "narrow", None),
            P("wide", "narrow", None, None),
            P(("wide", "narrow"), None),
        ),
        out_specs=(P(None, "wide", "narrow", None), P(None, "wide", "narrow", None)),
        check_vma=False,
    )
```

```python
import functools

import jax
import jax.numpy as jnp
from jax import lax
from jax.experimental import pallas as pl
from jax.experimental.pallas import tpu as pltpu
from jax.sharding import PartitionSpec as P

SWEEPS = 3
HIGHEST = lax.Precision.HIGHEST
NT = (((1,), (1,)), ((), ()))
F32 = jnp.float32

DIRS = ((-1, 0), (1, 0), (0, -1), (0, 1), (-1, -1), (-1, 1), (1, -1), (1, 1))


def halo_piece(d, px, cy, depth_x, depth_y):
    dx, dy = d
    if dx == 0:
        sp, dp, npair = 2, 2, px
    elif dx > 0:
        sp, dp, npair = 2 + px - depth_x, 2 - depth_x, depth_x
    else:
        sp, dp, npair = 2, 2 + px, depth_x
    if dy == 0:
        sr, dr, nrow = 0, 0, cy
    elif dy > 0:
        sr, dr, nrow = cy - depth_y, 2 * cy - depth_y, depth_y
    else:
        sr, dr, nrow = 0, cy, depth_y
    return (pl.ds(sp, npair), pl.ds(sr, nrow)), (pl.ds(dp, npair), pl.ds(dr, nrow))


def body(
    nw, nn,
    rhs, start, trans, accum, coupling, cells, widx, agg, tiles, cinv,
    out_it, out_res,
    COEF, CUR, FIX, W1, W2, H, DER, TF, CI, AG, AGX, ACC, GB, YB,
    loc, hs, hr, cs, cr, gs, gr, is_, ir,
):
    phases = rhs.shape[0]
    px, cy, tile = accum.shape
    box = px + 2
    half = tile // 2
    aggs = CI.shape[0]
    me_w, me_n = lax.axis_index("wide"), lax.axis_index("narrow")

    def dev(dw, dn):
        return {"wide": lax.rem(me_w + dw + nw, nw), "narrow": lax.rem(me_n + dn + nn, nn)}

    own = pl.ds(2, px)
    top = pl.ds(0, cy)
    nch = COEF.shape[0]
    first_rhs = nch - phases
    copies = [
        (accum, ACC),
        (trans, COEF.at[pl.ds(0, 3), own, top]),
        (start, CUR.at[0, :, own, top]),
        (coupling, COEF.at[pl.ds(4, phases * phases), own, top]),
        (rhs, COEF.at[pl.ds(first_rhs, phases), own, top]),
        (agg, AG),
        (cinv, CI),
        (tiles, TF),
    ]
    local = [pltpu.make_async_copy(s, d, loc.at[k]) for k, (s, d) in enumerate(copies)]
    for c in local:
        c.start()

    barrier = pltpu.get_barrier_semaphore()
    peers = [(dw, dn) for dw in range(nw) for dn in range(nn) if dw or dn]
    for p in range(px + 4):
        AGX[p] = jnp.zeros((2 * cy, tile), jnp.int32)
    for d in peers:
        pl.semaphore_signal(barrier, inc=1, device_id=dev(*d), device_id_type=pl.DeviceIdType.MESH)

    conn = cells.shape[-1]
    cell_row = cells[...]
    rows_own = px * cy
    hit_r = lax.broadcasted_iota(jnp.int32, (rows_own, conn), 0) == cell_row // tile
    hit_l = lax.broadcasted_iota(jnp.int32, (tile, conn), 0) == cell_row % tile
    left = jnp.where(hit_r, jnp.broadcast_to(widx[...], (rows_own, conn)), 0.0)
    right = jnp.where(hit_l, 1.0, 0.0)
    wells = lax.dot_general(left, right, NT, precision=HIGHEST, preferred_element_type=F32)
    local[0].wait()
    COEF[3, 2 : 2 + px, 0:cy, :] = ACC[...] + wells.reshape(px, cy, tile)
    for c in local[1:5]:
        c.wait()
    pl.semaphore_wait(barrier, len(peers))

    def remote(src, dst, ss, rs, d):
        return pltpu.make_async_remote_copy(
            src_ref=src, dst_ref=dst, send_sem=ss, recv_sem=rs,
            device_id=dev(*d), device_id_type=pl.DeviceIdType.MESH,
        )

    def halo(e):
        out = []
        for k, d in enumerate(DIRS):
            src, dst = halo_piece(d, px, cy, 2, 2 if d[0] else 3)
            out.append(remote(CUR.at[(e, slice(None)) + src], CUR.at[(e, slice(None)) + dst],
                              hs.at[e, k], hr.at[e, k], d))
        return out

    coef = []

    def send_coef(channels, src, dst, d):
        k = len(coef)
        coef.append(remote(COEF.at[(channels,) + src], COEF.at[(channels,) + dst], cs.at[k], cr.at[k], d))

    for d in DIRS:
        depth_y = 1 if d[0] < 0 else 2
        src, dst = halo_piece(d, px, cy, 1, depth_y)
        send_coef(pl.ds(0, nch), src, dst, d)
        if d[0] > 0:
            (_, sr), (_, dr) = src, dst
            send_coef(pl.ds(0, 1), (pl.ds(px, 1), sr), (pl.ds(0, 1), dr), d)
        if d[1] > 0:
            (sp, _), (dp, _) = src, dst
            send_coef(pl.ds(1, 1), (sp, pl.ds(cy - depth_y - 1, 1)), (dp, pl.ds(2 * cy - depth_y - 1, 1)), d)

    aggregates = []
    for k, d in enumerate(DIRS):
        src, dst = halo_piece(d, px, cy, 2, 2 if d[0] else 3)
        aggregates.append(remote(AGX.at[src], AGX.at[dst], is_.at[k], ir.at[k], d))
    for c in halo(0) + coef:
        c.start()
    local[5].wait()
    AGX[2 : 2 + px, 0:cy] = (AG[...] + me_n * aggs).reshape(px, cy, tile)
    for c in aggregates:
        c.start()

    lane = lax.broadcasted_iota(jnp.int32, (2 * cy, tile), 1)
    low = lane < half
    roll = pltpu.roll

    zero16 = jnp.zeros((2 * cy, tile), F32)
    for c in range(phases):
        for w in (W1, W2):
            w[c, 0] = zero16
            w[c, box + 1] = zero16
        W2[c, 1] = zero16
        W2[c, box] = zero16
    for c in local[6:]:
        c.wait()
    for c in coef:
        c.wait_recv()

    for b in range(box):
        tx = COEF[0, b + 1]
        txw = jnp.where(low, roll(COEF[0, b], half, 1), roll(tx, half, 1))
        ty = COEF[1, b + 1]
        tys = roll(ty, 1, 0)
        tz = jnp.where(lane % half < half - 1, COEF[2, b + 1], 0.0)
        tzd = roll(tz, 1, 1)
        centre = COEF[3, b + 1] + (tx + txw + ty + tys + tz + tzd)
        DER[0, b] = txw
        DER[1, b] = tys
        DER[2, b] = tz
        DER[3, b] = tzd
        for c in range(phases):
            diag = centre + COEF[4 + c * phases + c, b + 1]
            DER[4 + c, b] = diag
            DER[4 + phases + c, b] = 1.0 / diag

    def operate(read, boxes):
        swapped = {}

        def swap(c, idx):
            if (c, idx) not in swapped:
                swapped[c, idx] = roll(read(c, idx), half, 1)
            return swapped[c, idx]

        for b in boxes:
            values = [read(c, b + 1) for c in range(phases)]
            result = []
            for c in range(phases):
                v = values[c]
                east = jnp.where(low, swap(c, b + 1), swap(c, b + 2))
                west = jnp.where(low, swap(c, b), swap(c, b + 1))
                total = DER[4 + c, b] * v
                for o in range(phases):
                    if o != c:
                        total = total + COEF[4 + c * phases + o, b + 1] * values[o]
                inflow = COEF[0, b + 1] * east + DER[0, b] * west
                inflow = inflow + COEF[1, b + 1] * roll(v, 2 * cy - 1, 0)
                inflow = inflow + DER[1, b] * roll(v, 1, 0)
                inflow = inflow + DER[2, b] * roll(v, tile - 1, 1)
                inflow = inflow + DER[3, b] * roll(v, 1, 1)
                result.append(total - inflow)
            yield b, result

    row = lax.broadcasted_iota(jnp.int32, (phases * cy, tile), 0) % cy

    def product(b, q, chosen):
        stack = jnp.concatenate(q, axis=0)
        lhs = jnp.concatenate(
            [jnp.where(row == r, stack, 0.0) for r, _ in chosen], axis=1).astype(jnp.bfloat16)
        factors = jnp.concatenate([TF[b, t] for _, t in chosen], axis=1)
        out = lax.dot_general(lhs, factors, NT, preferred_element_type=F32)
        return [out[c * cy : (c + 1) * cy] for c in range(phases)]

    ring_a = tuple((y, y + 2) for y in range(cy))
    ring_b = ((0, cy + 2), (1, cy + 3), (cy - 2, 0), (cy - 1, 1))
    near_b = ((0, cy + 2), (cy - 1, 1))
    inner = range(1, box - 1)

    def scaled(b, h):
        return [DER[4 + phases + c, b] * h[c] for c in range(phases)]

    agg_iota = lax.broadcasted_iota(jnp.int32, (aggs, tile), 0)

    def current(e):
        return lambda c, idx: FIX[idx] if c == 0 else CUR[e, c, idx]

    def sweep(s, carry):
        read = current(s)
        acc = jnp.zeros((aggs, tile), F32)
        for b, applied in operate(read, inner):
            h = [COEF[first_rhs + c, b + 1] - applied[c] for c in range(phases)]
            for c in range(phases):
                H[c, b] = h[c]
            if True:
                for y in range(cy):
                    ids = AG[pl.ds((b - 1) * cy + y, 1), :]
                    acc = acc + jnp.where(agg_iota == ids, h[0][y : y + 1], 0.0)
        sums = jnp.broadcast_to(jnp.sum(acc, axis=1, keepdims=True), (aggs, tile))
        for g in range(nw):
            y = jnp.sum(CI[:, g * tile : (g + 1) * tile] * sums, axis=0, keepdims=True)
            for k in range(3):
                YB[s, (g + 1 - k) % nw, k : k + 1] = y
        share = [remote(YB.at[s, lax.rem(me_w + d[0], nw)], GB.at[s, k], gs.at[k], gr.at[s, k], d)
                 for k, d in enumerate(peers)]
        for c in share:
            c.start()
        for b, applied in operate(read, (0, box - 1)):
            for c in range(phases):
                H[c, b] = COEF[first_rhs + c, b + 1] - applied[c]

        for b in range(box):
            q = scaled(b, [H[c, b] for c in range(phases)])
            upper = product(b, [v[:cy] for v in q], ring_a)
            lower = product(b, [v[cy:] for v in q], ring_b if b in inner else near_b)
            for c in range(phases):
                W1[c, b + 1, 0:cy] = upper[c]
                W1[c, b + 1, cy : 2 * cy] = lower[c]

        for b, applied in operate(lambda c, idx: W1[c, idx], range(box)):
            q = scaled(b, [H[c, b] - applied[c] for c in range(phases)])
            upper = product(b, [v[:cy] for v in q], ring_a)
            for c in range(phases):
                W2[c, b + 1, 0:cy] = W1[c, b + 1, 0:cy] + upper[c]
            if b in inner:
                lower = product(b, [v[cy:] for v in q], near_b)
                for c in range(phases):
                    W2[c, b + 1, cy : 2 * cy] = W1[c, b + 1, cy : 2 * cy] + lower[c]

        for b, applied in operate(lambda c, idx: W2[c, idx], inner):
            q = scaled(b, [H[c, b] - applied[c] for c in range(phases)])
            upper = product(b, [v[:cy] for v in q], ring_a)
            for c in range(phases):
                W1[c, b + 1, 0:cy] = W2[c, b + 1, 0:cy] + upper[c]

        for c in range(phases):
            for p in range(px):
                CUR[s + 1, c, p + 2, 0:cy] = read(c, p + 2)[:cy] + W1[c, p + 2, 0:cy]
        for c in halo(s + 1):
            c.start()
        for c in share:
            c.wait_recv()
        total = YB[s, me_w]
        for k in range(len(peers)):
            total = total + GB[s, k]
        tables = [jnp.broadcast_to(total[k : k + 1], (2 * cy, tile)) for k in range(3)]
        for c in halo(s + 1):
            c.wait_recv()
        for p in range(px + 4):
            table = tables[0 if p < 2 else 1 if p < 2 + px else 2]
            lifted = jnp.take_along_axis(table, AGX[p], axis=1, mode="promise_in_bounds")
            FIX[p] = CUR[s + 1, 0, p] + lifted
        for c in share + halo(s):
            c.wait_send()
        return carry

    for c in halo(0):
        c.wait_recv()
    for p in range(px + 4):
        FIX[p] = CUR[0, 0, p]
    for c in aggregates:
        c.wait_recv()
    lax.fori_loop(0, SWEEPS, sweep, 0)
    last = current(SWEEPS)
    for c in range(phases):
        for p in range(px):
            out_it[c, p] = last(c, p + 2)[:cy]
    for b, applied in operate(last, inner):
        for c in range(phases):
            out_res[c, b - 1] = COEF[first_rhs + c, b + 1, 0:cy] - applied[c][:cy]
    for c in halo(SWEEPS) + coef + aggregates:
        c.wait_send()


def hand_over(iterate, residual, out_it, out_res):
    out_it[...] = iterate[...]
    out_res[...] = residual[...]


def solution(mesh):
    nw, nn = mesh.shape["wide"], mesh.shape["narrow"]

    def per_device(rhs, start, trans, accum, coupling, well_cells, well_index, agg_map, tile_factors, coarse_inverse):
        phases, px, cy, tile = rhs.shape
        box = px + 2
        aggs = coarse_inverse.shape[0]
        nch = 4 + phases * phases + phases
        vmem = pl.BlockSpec(memory_space=pltpu.VMEM)
        hbm = pl.BlockSpec(memory_space=pl.ANY)
        shape = jax.ShapeDtypeStruct(rhs.shape, F32)
        ring = (2 * cy, tile)
        dma = pltpu.SemaphoreType.DMA
        call = pl.pallas_call(
            functools.partial(body, nw, nn),
            out_shape=(shape, shape),
            in_specs=[hbm, hbm, hbm, hbm, hbm, vmem, vmem, hbm, hbm, hbm],
            out_specs=(vmem, vmem),
            scratch_shapes=[
                pltpu.VMEM((nch, px + 4) + ring, F32),
                pltpu.VMEM((SWEEPS + 1, phases, px + 4) + ring, F32),
                pltpu.VMEM((px + 4,) + ring, F32),
                pltpu.VMEM((phases, px + 4) + ring, F32),
                pltpu.VMEM((phases, px + 4) + ring, F32),
                pltpu.VMEM((phases, box) + ring, F32),
                pltpu.VMEM((4 + 2 * phases, box) + ring, F32),
                pltpu.VMEM(tile_factors.shape, tile_factors.dtype),
                pltpu.VMEM(coarse_inverse.shape, F32),
                pltpu.VMEM((px * cy, tile), jnp.int32),
                pltpu.VMEM((px + 4,) + ring, jnp.int32),
                pltpu.VMEM(accum.shape, F32),
                pltpu.VMEM((SWEEPS, nw * nn - 1, 3, tile), F32),
                pltpu.VMEM((SWEEPS, nw, 3, tile), F32),
                dma((8,)),
                dma((SWEEPS + 1, len(DIRS))),
                dma((SWEEPS + 1, len(DIRS))),
                dma((14,)),
                dma((14,)),
                dma((nw * nn - 1,)),
                dma((SWEEPS, nw * nn - 1)),
                dma((len(DIRS),)),
                dma((len(DIRS),)),
            ],
            compiler_params=pltpu.CompilerParams(collective_id=0, has_side_effects=True),
            name="schwarz",
        )
        held = call(
            rhs, start, trans, accum,
            coupling.reshape((phases * phases,) + accum.shape),
            well_cells.reshape(1, -1), well_index.reshape(1, -1),
            agg_map.reshape(px * cy, tile), tile_factors, coarse_inverse)
        return pl.pallas_call(
            hand_over, out_shape=(shape, shape), in_specs=[vmem, vmem], out_specs=(vmem, vmem),
            name="hand_over",
        )(*held)

    return jax.shard_map(
        per_device,
        mesh=mesh,
        in_specs=(
            P(None, "wide", "narrow", None),
            P(None, "wide", "narrow", None),
            P(None, "wide", "narrow", None),
            P("wide", "narrow", None),
            P(None, None, "wide", "narrow", None),
            P("wide", "narrow", None),
            P("wide", "narrow", None),
            P("wide", "narrow", None),
            P("wide", "narrow", None, None),
            P(("wide", "narrow"), None),
        ),
        out_specs=(P(None, "wide", "narrow", None), P(None, "wide", "narrow", None)),
        check_vma=False,
    )
```
